256 devices in a mesh: layer: 128 (over y_lo, x, z, core), src: 2 (over y_hi).
Axes of the slice: x: 4, y: 4 (y_hi: 2, y_lo: 2; y = y_hi * 2 + y_lo), z: 8, core: 2. Of those that a mesh axis runs over, the one named last changes fastest.
Arguments:
- down_maps: bfloat16 [128, 1664, 1664], P('layer'), may hold values from -1 to 1
- up_maps: bfloat16 [128, 1664, 1664], P('layer'), may hold values from -1 to 1
- local_traces: bfloat16 [128, 1664], P('src'), may hold values from -6 to 6
- src_depth: int32 [128], P('src'), may hold values from 0 to 127
Outputs:
- traces: bfloat16 [128, 128, 1664], P('layer', 'src')
- residual: bfloat16 [128, 128, 1664], P('layer', 'src')
The draws below stay inside these ranges and needn't reach their ends.
All inputs are finite; a program needn't handle non-finite values.
Results may differ from the reference program's by a relative error of at most 0.035.
Values may be sent and summed in bfloat16 or wider, within the bound.
No kernel may reach another device: no remote copies, remote signals or barrier semaphores. Data moves between devices by JAX's collectives and lax.ppermute only.
A program may use at most 64 MiB of HBM per device.

```python
import jax
import jax.numpy as jnp
from jax import lax

W = 1664
LAYER_TOTAL = 128
SOURCES = 128


coupling = 0.2


def transfer_maps(key, salt):
    random_child_keys = jax.random.split(jax.random.fold_in(key, salt), 6)
    slow_share = 0.5
    gentle_mask = jax.random.uniform(random_child_keys[0], (W,)) < slow_share
    slow_rate = jnp.exp(jax.random.uniform(random_child_keys[1], (W,), jnp.float32, jnp.log(0.2), jnp.log(1.0)))
    layer_spread = jnp.exp(jax.random.uniform(random_child_keys[2], (LAYER_TOTAL, 1), jnp.float32, jnp.log(0.7), jnp.log(1.4)))
    gentle_amplitude = jnp.sqrt(jnp.maximum(jnp.exp(-2.0 * slow_rate[None, :] * layer_spread / LAYER_TOTAL) - 0.5 * coupling * coupling, 0.01))
    quick_amplitude = jnp.exp(jax.random.uniform(random_child_keys[3], (LAYER_TOTAL, W), jnp.float32, jnp.log(0.3), jnp.log(0.8)))
    spike_layer_list = jax.random.randint(random_child_keys[4], (3,), 0, LAYER_TOTAL)
    spike_selected = jnp.any(jnp.arange(LAYER_TOTAL)[:, None] == spike_layer_list[None, :], axis=1)
    spike_scale = jnp.where(spike_selected[:, None], 0.7, 1.0)
    diagonal_amplitude = jnp.where(gentle_mask[None, :], gentle_amplitude * spike_scale, quick_amplitude)
    identity = jnp.eye(W, dtype=jnp.float32)
    mixing = jax.random.normal(random_child_keys[5], (LAYER_TOTAL, W, W), jnp.float32) * (coupling / jnp.sqrt(jnp.float32(W)))
    mixing = jnp.clip(mixing, -0.9, 0.9)
    return (mixing * (1.0 - identity) + diagonal_amplitude[:, :, None] * identity).astype(jnp.bfloat16)


def draw_down_maps(key, part):
    return transfer_maps(key, 11)


def draw_up_maps(key, part):
    return transfer_maps(key, 23)


def place_ends(drawn, own_key, least, top_value):
    longest = drawn.shape.index(max(drawn.shape))
    spots = []
    for shift in (0, 1):
        where = [jax.random.randint(jax.random.fold_in(own_key, axis), (), 0, length) for axis, length in enumerate(drawn.shape)]
        where[longest] = (where[longest] + shift) % drawn.shape[longest]
        spots.append(tuple(where))
    return drawn.at[spots[0]].set(least).at[spots[1]].set(top_value)


def block_levels(stream_key, extent, pieces, smallest, largest):
    gain, own = 1.0, jax.random.fold_in(stream_key, 6)
    for position, shards_of in pieces:
        steps = jnp.exp(jax.random.uniform(jax.random.fold_in(own, position), (shards_of,), jnp.float32, smallest / len(pieces), largest / len(pieces)))
        gain = gain * jnp.repeat(steps, extent[position] // shards_of).reshape([-1 if axis == position else 1 for axis in range(len(extent))])
    return gain


def gaussian(key, extent, width, limit, cuts=(), kind=jnp.bfloat16):
    result = jax.random.normal(key, extent, jnp.float32) * width
    if len(cuts) > 0:
        result = block_levels(key, extent, cuts, -0.22, 0.18) * result
    return jnp.clip(result, min=-limit, max=limit).astype(kind)


def setup_inputs(seed: int = 0) -> dict:
    splits = jax.random.split(jax.random.key(seed), 5)
    return {
        "down_maps": draw_down_maps(jax.random.fold_in(splits[4], 71), 0),
        "up_maps": draw_up_maps(jax.random.fold_in(splits[4], 71), 0),
        "local_traces": gaussian(splits[2], (SOURCES, W), 1.0, 6.0, ((0, 2),)),
        "src_depth": place_ends(jax.random.randint(splits[3], (SOURCES,), 0, LAYER_TOTAL), jax.random.fold_in(splits[3], 1), 0, LAYER_TOTAL - 1).astype(jnp.int32),
    }


def reference(down_maps, up_maps, local_traces, src_depth):
    layer_ids = jnp.arange(down_maps.shape[0], dtype=jnp.int32)
    placed = src_depth[None, :] == layer_ids[:, None]
    forcing = jnp.where(placed[:, :, None], local_traces.astype(jnp.float32)[None], jnp.float32(0.0))
    empty_edge = jnp.zeros(local_traces.shape, jnp.bfloat16)

    def sweep_step(state_edge, inputs):
        one_map, one_forcing = inputs
        fresh = one_forcing + jnp.dot(state_edge, one_map, preferred_element_type=jnp.float32)
        return fresh.astype(jnp.bfloat16), fresh

    _, downward = lax.scan(sweep_step, empty_edge, (down_maps, forcing))
    _, upward = lax.scan(sweep_step, empty_edge, (up_maps, forcing), reverse=True)
    combined = downward + upward - forcing
    rounded = combined.astype(jnp.bfloat16)
    zero_layer = jnp.zeros((1,) + rounded.shape[1:], jnp.bfloat16)
    above = jnp.concatenate([zero_layer, rounded[:-1]], axis=0)
    below = jnp.concatenate([rounded[1:], zero_layer], axis=0)

    def neighbour_terms(inputs):
        above_one, below_one, down_one, up_one = inputs
        first = jnp.dot(above_one.astype(jnp.float32), down_one.astype(jnp.float32))
        second = jnp.dot(below_one.astype(jnp.float32), up_one.astype(jnp.float32))
        return first, second

    from_above, from_below = lax.map(neighbour_terms, (above, below, down_maps, up_maps))
    remainder = forcing - combined + from_above + from_below
    return rounded, remainder.astype(jnp.bfloat16)
```

```python
import jax
import jax.numpy as jnp
from jax import lax
from jax.experimental import pallas as pl
from jax.experimental.pallas import tpu as pltpu
from jax.sharding import PartitionSpec as P

BF = jnp.bfloat16
F32 = jnp.float32
SINGLES = 12
PAIRS = 32
VMEM = pl.BlockSpec(memory_space=pltpu.VMEM)
SMEM = pl.BlockSpec(memory_space=pltpu.SMEM)
HBM = pl.BlockSpec(memory_space=pl.ANY)


def limit(mib):
    return pltpu.CompilerParams(vmem_limit_bytes=mib * 2**20)


def dot(a, b):
    return jnp.dot(a, b, preferred_element_type=F32)


def by_block(extent, block, body):
    whole = extent // block

    def step(i, carry):
        body(pl.multiple_of(i * block, block), block)
        return carry

    lax.fori_loop(0, whole, step, 0)
    if extent % block:
        body(whole * block, extent % block)


def pick(meta, down, up):
    def kernel(meta_ref, down_ref, up_ref, send_ref, own_ref, sems):
        def copies(first, second):
            one = pltpu.make_async_copy(first, send_ref, sems.at[0])
            two = pltpu.make_async_copy(second, own_ref, sems.at[1])
            one.start()
            two.start()
            one.wait()
            two.wait()

        @pl.when(meta_ref[2] == 0)
        def _():
            copies(down_ref, up_ref)

        @pl.when(meta_ref[2] != 0)
        def _():
            copies(up_ref, down_ref)

    shape = jax.ShapeDtypeStruct(down.shape, BF)
    return pl.pallas_call(
        kernel,
        out_shape=(shape, shape),
        in_specs=[SMEM, HBM, HBM],
        out_specs=(VMEM, VMEM),
        scratch_shapes=[pltpu.SemaphoreType.DMA((2,))],
        compiler_params=limit(14),
        name="pick",
    )(meta, down, up)


def product(meta, least, left, tail, right, right_tail, name):
    width = right.shape[1]
    rows = right_tail.shape[0] if right_tail is not None else right.shape[0] - width
    own_tail = tail is not None

    def kernel(meta_ref, *refs):
        refs = list(refs)
        out_ref = refs.pop()
        left_ref = refs.pop(0)
        tail_ref = refs.pop(0) if own_tail else None
        right_ref = refs.pop(0)
        add_ref = refs.pop(0) if right_tail is not None else None

        @pl.when(meta_ref[0] >= least)
        def _():
            def body(start, size):
                part = dot(left_ref[pl.ds(start, size), :], right_ref[0:width, :])
                out_ref[pl.ds(start, size), :] = part.astype(BF)

            by_block(width, 256, body)
            low = tail_ref[...] if own_tail else left_ref[width:, :]
            add = add_ref[...] if add_ref is not None else right_ref[width:, :]
            out_ref[width:, :] = (dot(low, right_ref[0:width, :]) + add.astype(F32)).astype(BF)

    args = [left] + ([tail] if own_tail else []) + [right] + ([right_tail] if right_tail is not None else [])
    return pl.pallas_call(
        kernel,
        out_shape=jax.ShapeDtypeStruct((width + rows, width), BF),
        in_specs=[SMEM] + [VMEM] * len(args),
        out_specs=VMEM,
        compiler_params=limit(24),
        name=name,
    )(meta, *args)


def advance(meta, position, arrived, maps, kept, out):
    rows, width = out.shape

    def kernel(meta_ref, x_ref, maps_ref, kept_in, out_in, kept_ref, out_ref):
        @pl.when(meta_ref[0] == position)
        def _():
            x = x_ref[...]
            kept_ref[...] = x

            def body(start, size):
                cols = pl.ds(start, size)
                part = dot(x, maps_ref[0:width, cols]) + maps_ref[width:, cols].astype(F32)
                out_ref[:, cols] = part.astype(BF)

            by_block(width, 256, body)

        @pl.when(meta_ref[0] != position)
        def _():
            kept_ref[...] = kept_in[...]
            out_ref[...] = out_in[...]

    shape = jax.ShapeDtypeStruct((rows, width), BF)
    return pl.pallas_call(
        kernel,
        out_shape=(shape, shape),
        in_specs=[SMEM] + [VMEM] * 4,
        out_specs=(VMEM, VMEM),
        compiler_params=limit(9),
        name="advance",
    )(meta, arrived, maps, kept, out)


def two_layers(x, maps1_ref, maps2_ref, add1_ref, add2_ref, first_ref, second_ref, leaving_ref, mid_ref):
    width = maps1_ref.shape[1]

    def body1(start, size):
        cols = pl.ds(start, size)
        part = dot(x, maps1_ref[:, cols]) + add1_ref[:, cols].astype(F32)
        first_ref[:, cols] = part
        mid_ref[:, cols] = part.astype(BF)

    by_block(width, 256, body1)
    mid = mid_ref[...]

    def body2(start, size):
        cols = pl.ds(start, size)
        part = dot(mid, maps2_ref[:, cols]) + add2_ref[:, cols].astype(F32)
        second_ref[:, cols] = part
        leaving_ref[:, cols] = part.astype(BF)

    by_block(width, 256, body2)


def settle_first(meta, kept, entering, entering_far, maps1, maps2, add1, add2, pair_maps):
    rows, width = kept.shape

    def kernel(meta_ref, kept_ref, near_ref, far_ref, m1, m2, a1, a2, pair_ref, first, second, leaving, mid):
        role = meta_ref[1]

        @pl.when(role == 0)
        def _():
            two_layers(kept_ref[...], m1, m2, a1, a2, first, second, leaving, mid)

        @pl.when(role == 1)
        def _():
            two_layers(near_ref[...], m1, m2, a1, a2, first, second, leaving, mid)

        @pl.when((role == 2) & (meta_ref[0] >= PAIRS))
        def _():
            x = far_ref[...]

            def body(start, size):
                cols = pl.ds(start, size)
                part = dot(x, pair_ref[0:width, cols]) + pair_ref[width:, cols].astype(F32)
                leaving[:, cols] = part.astype(BF)

            by_block(width, 256, body)

    return pl.pallas_call(
        kernel,
        out_shape=(
            jax.ShapeDtypeStruct((rows, width), F32),
            jax.ShapeDtypeStruct((rows, width), F32),
            jax.ShapeDtypeStruct((rows, width), BF),
        ),
        in_specs=[SMEM] + [VMEM] * 8,
        out_specs=(VMEM, VMEM, VMEM),
        scratch_shapes=[pltpu.VMEM((rows, width), BF)],
        compiler_params=limit(24),
        name="settle_first",
    )(meta, kept, entering, entering_far, maps1, maps2, add1, add2, pair_maps)


def settle(meta, roles, entering, maps1, maps2, add1, add2, first, second):
    rows, width = entering.shape

    def kernel(meta_ref, x_ref, m1, m2, a1, a2, first_in, second_in, first_ref, second_ref, leaving, mid):
        role = meta_ref[1]

        @pl.when((role >= roles[0]) & (role <= roles[1]))
        def _():
            two_layers(x_ref[...], m1, m2, a1, a2, first_ref, second_ref, leaving, mid)

        @pl.when((role < roles[0]) | (role > roles[1]))
        def _():
            first_ref[...] = first_in[...]
            second_ref[...] = second_in[...]

    return pl.pallas_call(
        kernel,
        out_shape=(
            jax.ShapeDtypeStruct((rows, width), F32),
            jax.ShapeDtypeStruct((rows, width), F32),
            jax.ShapeDtypeStruct((rows, width), BF),
        ),
        in_specs=[SMEM] + [VMEM] * 7,
        out_specs=(VMEM, VMEM, VMEM),
        scratch_shapes=[pltpu.VMEM((rows, width), BF)],
        compiler_params=limit(18),
        name="settle",
    )(meta, entering, maps1, maps2, add1, add2, first, second)


def finish(combined, own_add, partner, outer, maps_partner, maps_outer):
    rows, width = combined.shape

    def kernel(c_ref, a_ref, x_ref, o_ref, m1, m2, out_ref):
        x = x_ref[...]
        o = o_ref[...]

        def body(start, size):
            cols = pl.ds(start, size)
            part = dot(x, m1[:, cols]) + dot(o, m2[:, cols])
            out_ref[:, cols] = (a_ref[:, cols].astype(F32) - c_ref[:, cols] + part).astype(BF)

        by_block(width, 256, body)

    return pl.pallas_call(
        kernel,
        out_shape=jax.ShapeDtypeStruct((rows, width), BF),
        in_specs=[VMEM] * 6,
        out_specs=VMEM,
        compiler_params=limit(18),
        name="finish",
    )(combined, own_add, partner, outer, maps_partner, maps_outer)


def shards(down_maps, up_maps, local_traces, src_depth):
    down, up = down_maps[0], up_maps[0]
    rows, width = local_traces.shape
    count = lax.axis_size("layer")
    chips = count // 2
    layer = lax.axis_index("layer")
    core = layer % 2
    chip = layer // 2
    position = jnp.where(core == 1, chip, chips - 1 - chip)
    role = jnp.where(
        position < SINGLES,
        0,
        jnp.where(position < PAIRS, 1 + (position - SINGLES) % 2, 1 + (position - PAIRS) % 4),
    )
    meta = jnp.stack([position, role, core]).astype(jnp.int32)

    def device(at):
        return (2 * at + 1, 2 * (chips - 1 - at))

    def links(steps):
        return [pair for a, b in steps for pair in zip(device(a), device(b))]

    def move(value, steps):
        return lax.ppermute(value, "layer", links(steps))

    partners = [(i, i ^ 1) for i in range(count)]
    zero = jnp.zeros((), BF)
    add2 = jnp.where((src_depth == layer)[:, None], local_traces, zero)
    add1 = jnp.where((src_depth == layer + 1 - 2 * core)[:, None], local_traces, zero)

    given, maps2 = pick(meta, down, up)
    maps1 = lax.ppermute(given, "layer", partners)
    one = product(meta, 0, maps1, add1, maps2, add2, "chip_product")
    evens = range(SINGLES, chips, 2)
    two = product(meta, SINGLES, move(one, [(e, e + 1) for e in evens]), None, one, None, "pair_product")
    quads = range(PAIRS, chips, 4)
    four = product(meta, PAIRS, move(two, [(e + 1, e + 3) for e in quads]), None, two, None, "quad_product")

    stops = [(at, one) for at in range(SINGLES)]
    stops += [(e + 1, two) for e in range(SINGLES, PAIRS, 2)]
    stops += [(e + 3, four) for e in range(PAIRS, chips - 4, 4)]
    blank = jnp.zeros((rows, width), BF)
    arrived, kept, out = blank, blank, blank
    last = None
    for at, maps in stops:
        if last is not None:
            arrived = move(out, [(last, at)])
        kept, out = advance(meta, at, arrived, maps, kept, out)
        last = at

    firsts = list(range(SINGLES, PAIRS, 2)) + list(quads)
    near = move(out, [(e - 1, e) for e in firsts])
    far = move(out, [(e - 1, e + 1) for e in quads])
    first, second, leaving = settle_first(meta, kept, near, far, maps1, maps2, add1, add2, two)
    entering = move(leaving, [(e, e + 1) for e in firsts] + [(e + 1, e + 2) for e in quads])
    first, second, leaving = settle(meta, (2, 3), entering, maps1, maps2, add1, add2, first, second)
    entering = move(leaving, [(e + 2, e + 3) for e in quads])
    first, second, leaving = settle(meta, (4, 4), entering, maps1, maps2, add1, add2, first, second)

    combined = second + lax.ppermute(first, "layer", partners) - add2.astype(F32)
    rounded = combined.astype(BF)
    partner = lax.ppermute(rounded, "layer", partners)
    outward = [(i, i + 1) for i in range(1, count - 1, 2)]
    outer = lax.ppermute(rounded, "layer", outward + [(b, a) for a, b in outward])
    residual = finish(combined, add2, partner, outer, maps2, given)
    return (rounded[None], residual[None])


def solution(mesh):
    placed = (P("layer", None, None), P("layer", None, None), P("src", None), P("src"))
    return jax.shard_map(
        shards,
        mesh=mesh,
        in_specs=placed,
        out_specs=(P("layer", "src", None), P("layer", "src", None)),
        check_vma=False,
    )
```

```python
import jax
import jax.numpy as jnp
from jax import lax
from jax.experimental import pallas as pl
from jax.experimental.pallas import tpu as pltpu
from jax.sharding import PartitionSpec as P

BF = jnp.bfloat16
F32 = jnp.float32
EARLY = 3
SINGLES = 12
PAIRS = 24
VMEM = pl.BlockSpec(memory_space=pltpu.VMEM)
SMEM = pl.BlockSpec(memory_space=pltpu.SMEM)
HBM = pl.BlockSpec(memory_space=pltpu.HBM)


def limit(mib):
    return pltpu.CompilerParams(vmem_limit_bytes=mib * 2**20)


def dot(a, b):
    return jnp.dot(a, b, preferred_element_type=F32)


def by_block(extent, block, body):
    whole = extent // block

    def step(i, carry):
        body(pl.multiple_of(i * block, block), block)
        return carry

    lax.fori_loop(0, whole, step, 0)
    if extent % block:
        body(whole * block, extent % block)


def cuts(width):
    step = -(-width // 2 // 256) * 256
    return [(0, step), (step, width)]


def through(x, parts):
    width = x.shape[1]
    spans = cuts(width)
    total = parts[-1][spans[-1][1] - spans[-1][0] :, :].astype(F32)
    for (low, high), part in zip(spans, parts):
        total = total + dot(x[:, low:high], part[0 : high - low, :])
    return total


def pick(meta, on_zero, on_one, name):
    def kernel(meta_ref, zero_ref, one_ref, out_ref, sem):
        @pl.when(meta_ref[2] == 0)
        def _():
            pltpu.sync_copy(zero_ref, out_ref)

        @pl.when(meta_ref[2] != 0)
        def _():
            pltpu.sync_copy(one_ref, out_ref)

    return pl.pallas_call(
        kernel,
        out_shape=pltpu.VMEM(on_zero.shape, BF),
        in_specs=[SMEM, HBM, HBM],
        out_specs=VMEM,
        scratch_shapes=[pltpu.SemaphoreType.DMA],
        compiler_params=limit(8),
        name=name,
    )(meta, on_zero, on_one)


def chip_product(meta, least, index, maps1, add1, maps2, add2):
    rows, width = add1.shape
    low, high = cuts(width)[index]
    last = high == width

    size = high - low + (rows if last else 0)
    block = size // 4 if size % 64 == 0 and not last else size // 2

    def kernel(meta_ref, maps1_ref, add1_ref, maps2_ref, add2_ref, out_ref, left_ref):
        @pl.when(meta_ref[0] >= least)
        def _():
            if last:
                left_ref[0 : high - low, :] = maps1_ref[low:high, :]
                left_ref[high - low :, :] = add1_ref[...]

            def body(start, count):
                left = left_ref[pl.ds(start, count), :] if last else maps1_ref[pl.ds(low + start, count), :]
                out_ref[pl.ds(start, count), :] = dot(left, maps2_ref[...]).astype(BF)

            by_block(size, block, body)
            if last:
                state = out_ref[high - low :, :].astype(F32) + add2_ref[...].astype(F32)
                out_ref[high - low :, :] = state.astype(BF)

    return pl.pallas_call(
        kernel,
        out_shape=jax.ShapeDtypeStruct((size, width), BF),
        in_specs=[SMEM] + [VMEM] * 4,
        out_specs=VMEM,
        scratch_shapes=[pltpu.VMEM((size if last else 16, width), BF)],
        compiler_params=limit(18),
        name="chip_product",
    )(meta, maps1, add1, maps2, add2)


def joint_product(meta, least, index, left, parts, name):
    width = left.shape[1]
    low, high = cuts(width)[index]
    last = high == width
    size = left.shape[0]
    block = size // 4 if size % 64 == 0 and not last else size // 2

    def kernel(meta_ref, left_ref, *refs):
        out_ref = refs[-1]
        part_refs = refs[:-1]

        def times(x):
            total = None
            for (a, b), part in zip(cuts(width), part_refs):
                piece = dot(x[:, a:b], part[0 : b - a, :])
                total = piece if total is None else total + piece
            return total

        @pl.when(meta_ref[0] >= least)
        def _():
            def body(start, count):
                out_ref[pl.ds(start, count), :] = times(left_ref[pl.ds(start, count), :]).astype(BF)

            by_block(size, block, body)
            if last:
                own = part_refs[-1][high - low :, :].astype(F32)
                out_ref[high - low :, :] = (out_ref[high - low :, :].astype(F32) + own).astype(BF)

    return pl.pallas_call(
        kernel,
        out_shape=jax.ShapeDtypeStruct(left.shape, BF),
        in_specs=[SMEM] + [VMEM] * (1 + len(parts)),
        out_specs=VMEM,
        compiler_params=limit(12),
        name=name,
    )(meta, left, *parts)


def begin(meta, maps2, add1, add2):
    def kernel(meta_ref, maps2_ref, add1_ref, add2_ref, out_ref):
        @pl.when(meta_ref[0] == 0)
        def _():
            out_ref[...] = (dot(add1_ref[...], maps2_ref[...]) + add2_ref[...].astype(F32)).astype(BF)

        @pl.when(meta_ref[0] != 0)
        def _():
            out_ref[...] = jnp.zeros(out_ref.shape, BF)

    return pl.pallas_call(
        kernel,
        out_shape=jax.ShapeDtypeStruct(add1.shape, BF),
        in_specs=[SMEM] + [VMEM] * 3,
        out_specs=VMEM,
        compiler_params=limit(8),
        name="begin",
    )(meta, maps2, add1, add2)


def advance(meta, position, arrived, maps, kept, out, adds=None):
    def kernel(meta_ref, x_ref, kept_in, out_in, *refs):
        map_refs, (kept_ref, out_ref) = refs[:-2], refs[-2:]

        @pl.when(meta_ref[0] == position)
        def _():
            x = x_ref[...]
            kept_ref[...] = x
            if adds is None:
                out_ref[...] = through(x, map_refs).astype(BF)
            else:
                maps1_ref, maps2_ref, add1_ref, add2_ref = map_refs
                mid = (dot(x, maps1_ref[...]) + add1_ref[...].astype(F32)).astype(BF)
                out_ref[...] = (dot(mid, maps2_ref[...]) + add2_ref[...].astype(F32)).astype(BF)

        @pl.when(meta_ref[0] != position)
        def _():
            kept_ref[...] = kept_in[...]
            out_ref[...] = out_in[...]

    operands = list(maps) + list(adds or ())
    shape = jax.ShapeDtypeStruct(out.shape, BF)
    return pl.pallas_call(
        kernel,
        out_shape=(shape, shape),
        in_specs=[SMEM] + [VMEM] * (3 + len(operands)),
        out_specs=(VMEM, VMEM),
        compiler_params=limit(12),
        name="advance",
    )(meta, arrived, kept, out, *operands)


def relay(meta, entering, parts):
    def kernel(meta_ref, x_ref, *refs):
        @pl.when((meta_ref[1] == 2) & (meta_ref[0] >= PAIRS))
        def _():
            refs[-1][...] = through(x_ref[...], refs[:-1]).astype(BF)

    return pl.pallas_call(
        kernel,
        out_shape=jax.ShapeDtypeStruct(entering.shape, BF),
        in_specs=[SMEM] + [VMEM] * (1 + len(parts)),
        out_specs=VMEM,
        compiler_params=limit(8),
        name="relay",
    )(meta, entering, *parts)


def two_layers(x, maps1_ref, maps2_ref, add1_ref, add2_ref, first_ref, second_ref):
    first = dot(x, maps1_ref[...]) + add1_ref[...].astype(F32)
    first_ref[...] = first
    second_ref[...] = dot(first.astype(BF), maps2_ref[...]) + add2_ref[...].astype(F32)


def settle_most(meta, chips, kept, near, far, final, maps1, maps2, add1, add2, before1, before2):
    rows, width = kept.shape
    count = len(before1)

    def kernel(meta_ref, kept_ref, near_ref, far_ref, final_ref, m1, m2, a1, a2, *refs):
        part1, part2 = refs[:count], refs[count : 2 * count]
        first_ref, second_ref, x_ref = refs[2 * count :]
        position = meta_ref[0]
        role = meta_ref[1]
        from_near = role == 1
        from_far = (role == 2) & (position >= PAIRS)
        from_final = position == chips - 1

        @pl.when(from_near)
        def _():
            x_ref[...] = near_ref[...]

        @pl.when(from_far)
        def _():
            x_ref[...] = far_ref[...]

        @pl.when(from_final)
        def _():
            x_ref[...] = final_ref[...]

        @pl.when(jnp.logical_not(from_near | from_far | from_final))
        def _():
            x_ref[...] = kept_ref[...]

        @pl.when(role == 4)
        def _():
            x_ref[...] = through(x_ref[...], part2).astype(BF)

        @pl.when((role == 2) | (role == 4))
        def _():
            x_ref[...] = through(x_ref[...], part1).astype(BF)

        @pl.when(role != 3)
        def _():
            two_layers(x_ref[...], m1, m2, a1, a2, first_ref, second_ref)

    shape = jax.ShapeDtypeStruct((rows, width), F32)
    return pl.pallas_call(
        kernel,
        out_shape=(shape, shape),
        in_specs=[SMEM] + [VMEM] * (8 + 2 * count),
        out_specs=(VMEM, VMEM),
        scratch_shapes=[pltpu.VMEM((rows, width), BF)],
        compiler_params=limit(16),
        name="settle_most",
    )(meta, kept, near, far, final, maps1, maps2, add1, add2, *before1, *before2)


def settle_third(meta, entering, maps1, maps2, add1, add2, first, second):
    rows, width = entering.shape

    def kernel(meta_ref, x_ref, m1, m2, a1, a2, first_in, second_in, first_ref, second_ref):
        @pl.when(meta_ref[1] == 3)
        def _():
            two_layers(x_ref[...], m1, m2, a1, a2, first_ref, second_ref)

        @pl.when(meta_ref[1] != 3)
        def _():
            first_ref[...] = first_in[...]
            second_ref[...] = second_in[...]

    shape = jax.ShapeDtypeStruct((rows, width), F32)
    return pl.pallas_call(
        kernel,
        out_shape=(shape, shape),
        in_specs=[SMEM] + [VMEM] * 7,
        out_specs=(VMEM, VMEM),
        compiler_params=limit(16),
        name="settle_third",
    )(meta, entering, maps1, maps2, add1, add2, first, second)


def finish(combined, own_add, partner, outer, maps_partner, maps_outer):
    def kernel(c_ref, a_ref, x_ref, o_ref, m1, m2, out_ref):
        part = dot(x_ref[...], m1[...]) + dot(o_ref[...], m2[...])
        out_ref[...] = (a_ref[...].astype(F32) - c_ref[...] + part).astype(BF)

    return pl.pallas_call(
        kernel,
        out_shape=jax.ShapeDtypeStruct(combined.shape, BF),
        in_specs=[VMEM] * 6,
        out_specs=VMEM,
        compiler_params=limit(16),
        name="finish",
    )(combined, own_add, partner, outer, maps_partner, maps_outer)


def shards(down_maps, up_maps, local_traces, src_depth):
    down, up = down_maps[0], up_maps[0]
    rows, width = local_traces.shape
    count = lax.axis_size("layer")
    chips = count // 2
    layer = lax.axis_index("layer")
    core = layer % 2
    chip = layer // 2
    position = jnp.where(core == 1, chip, chips - 1 - chip)
    role = jnp.where(
        position < SINGLES,
        0,
        jnp.where(position < PAIRS, 1 + (position - SINGLES) % 2, 1 + (position - PAIRS) % 4),
    )
    meta = jnp.stack([position, role, core]).astype(jnp.int32)

    def device(at):
        return (2 * at + 1, 2 * (chips - 1 - at))

    def links(steps):
        return [pair for a, b in steps for pair in zip(device(a), device(b))]

    def move(value, steps):
        return lax.ppermute(value, "layer", links(steps))

    partners = [(i, i ^ 1) for i in range(count)]
    zero = jnp.zeros((), BF)
    add2 = jnp.where((src_depth == layer)[:, None], local_traces, zero)
    add1 = jnp.where((src_depth == layer + 1 - 2 * core)[:, None], local_traces, zero)

    down = pltpu.with_memory_space_constraint(down, pltpu.HBM)
    up = pltpu.with_memory_space_constraint(up, pltpu.HBM)
    given = pick(meta, down, up, "pick_given")
    maps2 = pick(meta, up, down, "pick_own")
    maps1 = pltpu.with_memory_space_constraint(lax.ppermute(given, "layer", partners), pltpu.VMEM)
    given = pltpu.with_memory_space_constraint(given, pltpu.VMEM)
    maps2 = pltpu.with_memory_space_constraint(maps2, pltpu.VMEM)
    thirds = range(len(cuts(width)))
    one = [chip_product(meta, EARLY, i, maps1, add1, maps2, add2) for i in thirds]
    pairs = [(e, e + 1) for e in range(SINGLES, chips, 2)]
    before1 = [move(part, pairs) for part in one]
    two = [joint_product(meta, SINGLES, i, before1[i], one, "pair_product") for i in thirds]
    quads = range(PAIRS, chips, 4)
    before2 = [move(part, [(e + 1, e + 3) for e in quads]) for part in two]
    four = [joint_product(meta, PAIRS, i, before2[i], two, "quad_product") for i in thirds]

    stops = [(at, None) for at in range(1, EARLY)]
    stops += [(at, one) for at in range(EARLY, SINGLES)]
    stops += [(e + 1, two) for e in range(SINGLES, PAIRS, 2)]
    stops += [(e + 3, four) for e in range(PAIRS, chips - 4, 4)]
    kept = jnp.zeros((rows, width), BF)
    out = begin(meta, maps2, add1, add2)
    last = 0
    for at, maps in stops:
        arrived = move(out, [(last, at)])
        if maps is None:
            kept, out = advance(meta, at, arrived, (maps1, maps2), kept, out, (add1, add2))
        else:
            kept, out = advance(meta, at, arrived, maps, kept, out)
        last = at

    far = move(out, [(e - 1, e + 1) for e in quads])
    final = move(out, [(last, chips - 1)])
    near = move(out, [(e - 1, e) for e in list(range(SINGLES, PAIRS, 2)) + list(quads)])
    passed = move(relay(meta, far, two), [(e + 1, e + 2) for e in quads])
    first, second = settle_most(
        meta, chips, kept, near, far, final, maps1, maps2, add1, add2, before1, before2
    )
    first, second = settle_third(meta, passed, maps1, maps2, add1, add2, first, second)

    combined = second + lax.ppermute(first, "layer", partners) - add2.astype(F32)
    rounded = combined.astype(BF)
    partner = lax.ppermute(rounded, "layer", partners)
    outward = [(i, i + 1) for i in range(1, count - 1, 2)]
    outer = lax.ppermute(rounded, "layer", outward + [(b, a) for a, b in outward])
    residual = finish(combined, add2, partner, outer, maps2, given)
    return (rounded[None], residual[None])


def solution(mesh):
    placed = (P("layer", None, None), P("layer", None, None), P("src", None), P("src"))
    return jax.shard_map(
        shards,
        mesh=mesh,
        in_specs=placed,
        out_specs=(P("layer", "src", None), P("layer", "src", None)),
        check_vma=False,
    )
```

```python
import jax
import jax.numpy as jnp
from jax import lax
from jax.experimental import pallas as pl
from jax.experimental.pallas import tpu as pltpu
from jax.sharding import PartitionSpec as P

BF = jnp.bfloat16
F32 = jnp.float32
EARLY = 1
SINGLES = 8
PAIRS = 24
VMEM = pl.BlockSpec(memory_space=pltpu.VMEM)
SMEM = pl.BlockSpec(memory_space=pltpu.SMEM)
HBM = pl.BlockSpec(memory_space=pltpu.HBM)


def limit(mib):
    return pltpu.CompilerParams(vmem_limit_bytes=mib * 2**20)


def dot(a, b):
    return jnp.dot(a, b, preferred_element_type=F32)


def by_block(extent, block, body):
    whole = extent // block

    def step(i, carry):
        body(pl.multiple_of(i * block, block), block)
        return carry

    if whole > 1:
        lax.fori_loop(0, whole, step, 0)
    else:
        body(0, block)
    if extent % block:
        body(whole * block, extent % block)


def cuts(width):
    step = -(-width // 2 // 256) * 256
    return [(0, step), (step, width)]


def through(x, parts):
    width = x.shape[1]
    spans = cuts(width)
    total = parts[-1][spans[-1][1] - spans[-1][0] :, :].astype(F32)
    for (low, high), part in zip(spans, parts):
        total = total + dot(x[:, low:high], part[0 : high - low, :])
    return total


def pick(meta, on_zero, on_one, name, after=None):
    first = () if after is None else (after,)

    def kernel(meta_ref, zero_ref, one_ref, *refs):
        out_ref = refs[len(first)]

        @pl.when(meta_ref[2] == 0)
        def _():
            pltpu.sync_copy(zero_ref, out_ref)

        @pl.when(meta_ref[2] != 0)
        def _():
            pltpu.sync_copy(one_ref, out_ref)

    return pl.pallas_call(
        kernel,
        out_shape=pltpu.VMEM(on_zero.shape, BF),
        in_specs=[SMEM, HBM, HBM] + [pl.BlockSpec(memory_space=pl.ANY)] * len(first),
        out_specs=VMEM,
        compiler_params=limit(8),
        name=name,
    )(meta, on_zero, on_one, *first)


def chip_product(meta, least, index, maps1, add1, maps2, add2):
    rows, width = add1.shape
    low, high = cuts(width)[index]
    last = high == width

    size = high - low + (rows if last else 0)
    block = 256 if not last else size // 4

    def kernel(meta_ref, maps1_ref, add1_ref, maps2_ref, add2_ref, out_ref, left_ref):
        @pl.when(meta_ref[0] >= least)
        def _():
            if last:
                left_ref[0 : high - low, :] = maps1_ref[low:high, :]
                left_ref[high - low :, :] = add1_ref[...]

            def body(start, count):
                left = left_ref[pl.ds(start, count), :] if last else maps1_ref[pl.ds(low + start, count), :]
                out_ref[pl.ds(start, count), :] = dot(left, maps2_ref[...]).astype(BF)

            by_block(size, block, body)
            if last:
                state = out_ref[high - low :, :].astype(F32) + add2_ref[...].astype(F32)
                out_ref[high - low :, :] = state.astype(BF)

    return pl.pallas_call(
        kernel,
        out_shape=jax.ShapeDtypeStruct((size, width), BF),
        in_specs=[SMEM] + [VMEM] * 4,
        out_specs=VMEM,
        scratch_shapes=[pltpu.VMEM((size if last else 16, width), BF)],
        compiler_params=limit(18),
        name="chip_product",
    )(meta, maps1, add1, maps2, add2)


def joint_product(meta, least, index, left, parts, name):
    width = left.shape[1]
    low, high = cuts(width)[index]
    last = high == width
    size = left.shape[0]
    block = 256 if not last else size // 4

    def kernel(meta_ref, left_ref, *refs):
        out_ref = refs[-1]
        part_refs = refs[:-1]

        def times(x):
            total = None
            for (a, b), part in zip(cuts(width), part_refs):
                piece = dot(x[:, a:b], part[0 : b - a, :])
                total = piece if total is None else total + piece
            return total

        @pl.when(meta_ref[0] >= least)
        def _():
            def body(start, count):
                out_ref[pl.ds(start, count), :] = times(left_ref[pl.ds(start, count), :]).astype(BF)

            by_block(size, block, body)
            if last:
                own = part_refs[-1][high - low :, :].astype(F32)
                out_ref[high - low :, :] = (out_ref[high - low :, :].astype(F32) + own).astype(BF)

    return pl.pallas_call(
        kernel,
        out_shape=jax.ShapeDtypeStruct(left.shape, BF),
        in_specs=[SMEM] + [VMEM] * (1 + len(parts)),
        out_specs=VMEM,
        compiler_params=limit(12),
        name=name,
    )(meta, left, *parts)


def begin(meta, maps2, add1, add2):
    def kernel(meta_ref, maps2_ref, add1_ref, add2_ref, out_ref):
        @pl.when(meta_ref[0] == 0)
        def _():
            value = add1_ref[...]

            def body(start, count):
                cols = pl.ds(start, count)
                out_ref[:, cols] = (dot(value, maps2_ref[:, cols]) + add2_ref[:, cols].astype(F32)).astype(BF)

            by_block(maps2_ref.shape[1], 512, body)

        @pl.when(meta_ref[0] != 0)
        def _():
            out_ref[...] = jnp.zeros(out_ref.shape, BF)

    return pl.pallas_call(
        kernel,
        out_shape=jax.ShapeDtypeStruct(add1.shape, BF),
        in_specs=[SMEM] + [VMEM] * 3,
        out_specs=VMEM,
        compiler_params=limit(8),
        name="begin",
    )(meta, maps2, add1, add2)


def advance(meta, position, arrived, maps, kept, out, block):
    def kernel(meta_ref, x_ref, kept_in, out_in, *refs):
        map_refs, (kept_ref, out_ref) = refs[:-2], refs[-2:]

        @pl.when(meta_ref[0] == position)
        def _():
            x = x_ref[...]
            kept_ref[...] = x
            width = x.shape[1]

            def body(start, count):
                cols = pl.ds(start, count)
                out_ref[:, cols] = through(x, [ref.at[:, cols] for ref in map_refs]).astype(BF)

            by_block(width, block, body)

        @pl.when(meta_ref[0] != position)
        def _():
            kept_ref[...] = kept_in[...]
            out_ref[...] = out_in[...]

    operands = list(maps)
    shape = jax.ShapeDtypeStruct(out.shape, BF)
    return pl.pallas_call(
        kernel,
        out_shape=(shape, shape),
        in_specs=[SMEM] + [VMEM] * (3 + len(operands)),
        out_specs=(VMEM, VMEM),
        compiler_params=limit(12),
        name="advance",
    )(meta, arrived, kept, out, *operands)


def late(maps, after, name):
    def kernel(maps_ref, after_ref, out_ref):
        pltpu.sync_copy(maps_ref, out_ref)

    return pl.pallas_call(
        kernel,
        out_shape=jax.ShapeDtypeStruct(maps.shape, BF),
        in_specs=[pl.BlockSpec(memory_space=pl.ANY)] * 2,
        out_specs=pl.BlockSpec(memory_space=pl.ANY),
        compiler_params=limit(8),
        name=name,
    )(maps, after)


def relay(meta, entering, parts):
    def kernel(meta_ref, x_ref, *refs):
        @pl.when((meta_ref[1] == 2) & (meta_ref[0] >= PAIRS))
        def _():
            refs[-1][...] = through(x_ref[...], refs[:-1]).astype(BF)

    return pl.pallas_call(
        kernel,
        out_shape=jax.ShapeDtypeStruct(entering.shape, BF),
        in_specs=[SMEM] + [VMEM] * (1 + len(parts)),
        out_specs=VMEM,
        compiler_params=limit(8),
        name="relay",
    )(meta, entering, *parts)


def two_layers(x, maps1_ref, maps2_ref, add1_ref, add2_ref, first_ref, second_ref):
    def layer(value, maps_ref, add_ref, out_ref):
        def body(start, count):
            cols = pl.ds(start, count)
            out_ref[:, cols] = dot(value, maps_ref[:, cols]) + add_ref[:, cols].astype(F32)

        by_block(maps_ref.shape[1], 512, body)

    layer(x, maps1_ref, add1_ref, first_ref)
    layer(first_ref[...].astype(BF), maps2_ref, add2_ref, second_ref)


def settle_most(meta, chips, kept, near, far, final, maps1, maps2, add1, add2, before1, before2):
    rows, width = kept.shape
    count = len(before1)

    def kernel(meta_ref, kept_ref, near_ref, far_ref, final_ref, m1, m2, a1, a2, *refs):
        part1, part2 = refs[:count], refs[count : 2 * count]
        first_ref, second_ref, x_ref = refs[2 * count :]
        position = meta_ref[0]
        role = meta_ref[1]
        from_near = role == 1

        def enter(parts):
            x = x_ref[...]

            def body(start, count):
                cols = pl.ds(start, count)
                x_ref[:, cols] = through(x, [ref.at[:, cols] for ref in parts]).astype(BF)

            by_block(width, 512, body)

        from_far = (role == 2) & (position >= PAIRS)
        from_final = position == chips - 1

        @pl.when(from_near)
        def _():
            x_ref[...] = near_ref[...]

        @pl.when(from_far)
        def _():
            x_ref[...] = far_ref[...]

        @pl.when(from_final)
        def _():
            x_ref[...] = final_ref[...]

        @pl.when(jnp.logical_not(from_near | from_far | from_final))
        def _():
            x_ref[...] = kept_ref[...]

        @pl.when(role == 4)
        def _():
            enter(part2)

        @pl.when((role == 2) | (role == 4))
        def _():
            enter(part1)

        @pl.when(role != 3)
        def _():
            two_layers(x_ref[...], m1, m2, a1, a2, first_ref, second_ref)

    shape = jax.ShapeDtypeStruct((rows, width), F32)
    return pl.pallas_call(
        kernel,
        out_shape=(shape, shape),
        in_specs=[SMEM] + [VMEM] * (8 + 2 * count),
        out_specs=(VMEM, VMEM),
        scratch_shapes=[pltpu.VMEM((rows, width), BF)],
        compiler_params=limit(16),
        name="settle_most",
    )(meta, kept, near, far, final, maps1, maps2, add1, add2, *before1, *before2)


def settle_third(meta, entering, maps1, maps2, add1, add2, first, second):
    rows, width = entering.shape

    def kernel(meta_ref, x_ref, m1, m2, a1, a2, first_in, second_in, first_ref, second_ref):
        @pl.when(meta_ref[1] == 3)
        def _():
            two_layers(x_ref[...], m1, m2, a1, a2, first_ref, second_ref)

        @pl.when(meta_ref[1] != 3)
        def _():
            first_ref[...] = first_in[...]
            second_ref[...] = second_in[...]

    shape = jax.ShapeDtypeStruct((rows, width), F32)
    return pl.pallas_call(
        kernel,
        out_shape=(shape, shape),
        in_specs=[SMEM] + [VMEM] * 7,
        out_specs=(VMEM, VMEM),
        compiler_params=limit(16),
        name="settle_third",
    )(meta, entering, maps1, maps2, add1, add2, first, second)


def finish(combined, own_add, partner, outer, maps_partner, maps_outer):
    def kernel(c_ref, a_ref, x_ref, o_ref, m1, m2, out_ref):
        part = dot(x_ref[...], m1[...]) + dot(o_ref[...], m2[...])
        out_ref[...] = (a_ref[...].astype(F32) - c_ref[...] + part).astype(BF)

    return pl.pallas_call(
        kernel,
        out_shape=jax.ShapeDtypeStruct(combined.shape, BF),
        in_specs=[VMEM] * 6,
        out_specs=VMEM,
        compiler_params=limit(16),
        name="finish",
    )(combined, own_add, partner, outer, maps_partner, maps_outer)


def shards(down_maps, up_maps, local_traces, src_depth):
    down, up = down_maps[0], up_maps[0]
    rows, width = local_traces.shape
    count = lax.axis_size("layer")
    chips = count // 2
    layer = lax.axis_index("layer")
    core = layer % 2
    chip = layer // 2
    position = jnp.where(core == 1, chip, chips - 1 - chip)
    role = jnp.where(
        position < SINGLES,
        0,
        jnp.where(position < PAIRS, 1 + (position - SINGLES) % 2, 1 + (position - PAIRS) % 4),
    )
    meta = jnp.stack([position, role, core]).astype(jnp.int32)

    def device(at):
        return (2 * at + 1, 2 * (chips - 1 - at))

    def links(steps):
        return [pair for a, b in steps for pair in zip(device(a), device(b))]

    def move(value, steps):
        return lax.ppermute(value, "layer", links(steps))

    partners = [(i, i ^ 1) for i in range(count)]
    zero = jnp.zeros((), BF)
    add2 = jnp.where((src_depth == layer)[:, None], local_traces, zero)
    add1 = jnp.where((src_depth == layer + 1 - 2 * core)[:, None], local_traces, zero)

    down = pltpu.with_memory_space_constraint(down, pltpu.HBM)
    up = pltpu.with_memory_space_constraint(up, pltpu.HBM)
    given = pick(meta, down, up, "pick_given")
    maps2 = pick(meta, up, down, "pick_own")
    maps1 = lax.ppermute(given, "layer", partners)
    thirds = range(len(cuts(width)))
    one = [chip_product(meta, EARLY, i, maps1, add1, maps2, add2) for i in thirds]
    pairs = [(e, e + 1) for e in range(SINGLES, chips, 2)]
    before1 = [move(part, pairs) for part in one]
    two = [joint_product(meta, SINGLES, i, before1[i], one, "pair_product") for i in thirds]
    quads = range(PAIRS, chips, 4)
    before2 = [move(part, [(e + 1, e + 3) for e in quads]) for part in two]
    four = [joint_product(meta, PAIRS, i, before2[i], two, "quad_product") for i in thirds]

    stops = [(at, one) for at in range(EARLY, SINGLES)]
    stops += [(e + 1, two) for e in range(SINGLES, PAIRS, 2)]
    stops += [(e + 3, four) for e in range(PAIRS, chips - 4, 4)]
    kept = jnp.zeros((rows, width), BF)
    out = begin(meta, maps2, add1, add2)
    last = 0
    for at, maps in stops:
        arrived = move(out, [(last, at)])
        if at == stops[-2][0]:
            ahead = out
        kept, out = advance(meta, at, arrived, maps, kept, out, width if maps is four else 512)
        last = at

    far = move(out, [(e - 1, e + 1) for e in quads])
    final = move(out, [(last, chips - 1)])
    near = move(out, [(e - 1, e) for e in list(range(SINGLES, PAIRS, 2)) + list(quads)])
    maps1 = late(maps1, ahead, "late_first")
    given = pick(meta, down, up, "late_given", ahead)
    passed = move(relay(meta, far, two), [(e + 1, e + 2) for e in quads])
    first, second = settle_most(
        meta, chips, kept, near, far, final, maps1, maps2, add1, add2, before1, before2
    )
    first, second = settle_third(meta, passed, maps1, maps2, add1, add2, first, second)

    combined = second + lax.ppermute(first, "layer", partners) - add2.astype(F32)
    rounded = combined.astype(BF)
    partner = lax.ppermute(rounded, "layer", partners)
    outward = [(i, i + 1) for i in range(1, count - 1, 2)]
    outer = lax.ppermute(rounded, "layer", outward + [(b, a) for a, b in outward])
    residual = finish(combined, add2, partner, outer, maps2, given)
    return (rounded[None], residual[None])


def solution(mesh):
    placed = (P("layer", None, None), P("layer", None, None), P("src", None), P("src"))
    return jax.shard_map(
        shards,
        mesh=mesh,
        in_specs=placed,
        out_specs=(P("layer", "src", None), P("layer", "src", None)),
        check_vma=False,
    )
```

```python
import jax
import jax.numpy as jnp
from jax import lax
from jax.experimental import pallas as pl
from jax.experimental.pallas import tpu as pltpu
from jax.sharding import PartitionSpec as P

BF = jnp.bfloat16
F32 = jnp.float32
EARLY = 1
SINGLES = 6
PAIRS = 24
VMEM = pl.BlockSpec(memory_space=pltpu.VMEM)
SMEM = pl.BlockSpec(memory_space=pltpu.SMEM)
HBM = pl.BlockSpec(memory_space=pltpu.HBM)


def limit(mib):
    return pltpu.CompilerParams(vmem_limit_bytes=mib * 2**20)


def dot(a, b):
    return jnp.dot(a, b, preferred_element_type=F32)


def by_block(extent, block, body):
    whole = extent // block

    def step(i, carry):
        body(pl.multiple_of(i * block, block), block)
        return carry

    if whole > 1:
        lax.fori_loop(0, whole, step, 0)
    else:
        body(0, block)
    if extent % block:
        body(whole * block, extent % block)


def cuts(width):
    step = -(-width // 2 // 256) * 256
    return [(0, step), (step, width)]


def through(x, parts):
    width = x.shape[1]
    spans = cuts(width)
    total = parts[-1][spans[-1][1] - spans[-1][0] :, :].astype(F32)
    for (low, high), part in zip(spans, parts):
        total = total + dot(x[:, low:high], part[0 : high - low, :])
    return total


def pick(meta, on_zero, on_one, name, after=None):
    first = () if after is None else (after,)

    def kernel(meta_ref, zero_ref, one_ref, *refs):
        out_ref = refs[len(first)]

        @pl.when(meta_ref[2] == 0)
        def _():
            pltpu.sync_copy(zero_ref, out_ref)

        @pl.when(meta_ref[2] != 0)
        def _():
            pltpu.sync_copy(one_ref, out_ref)

    return pl.pallas_call(
        kernel,
        out_shape=pltpu.VMEM(on_zero.shape, BF),
        in_specs=[SMEM, HBM, HBM] + [pl.BlockSpec(memory_space=pl.ANY)] * len(first),
        out_specs=VMEM,
        compiler_params=limit(8),
        name=name,
    )(meta, on_zero, on_one, *first)


def chip_product(meta, least, index, maps1, add1, maps2, add2):
    rows, width = add1.shape
    low, high = cuts(width)[index]
    last = high == width

    size = high - low + (rows if last else 0)
    block = 256 if not last else size // 4

    def kernel(meta_ref, maps1_ref, add1_ref, maps2_ref, add2_ref, out_ref, left_ref):
        @pl.when(meta_ref[0] >= least)
        def _():
            if last:
                left_ref[0 : high - low, :] = maps1_ref[low:high, :]
                left_ref[high - low :, :] = add1_ref[...]

            def body(start, count):
                left = left_ref[pl.ds(start, count), :] if last else maps1_ref[pl.ds(low + start, count), :]
                out_ref[pl.ds(start, count), :] = dot(left, maps2_ref[...]).astype(BF)

            by_block(size, block, body)
            if last:
                state = out_ref[high - low :, :].astype(F32) + add2_ref[...].astype(F32)
                out_ref[high - low :, :] = state.astype(BF)

    return pl.pallas_call(
        kernel,
        out_shape=jax.ShapeDtypeStruct((size, width), BF),
        in_specs=[SMEM] + [VMEM] * 4,
        out_specs=VMEM,
        scratch_shapes=[pltpu.VMEM((size if last else 16, width), BF)],
        compiler_params=limit(18),
        name="chip_product",
    )(meta, maps1, add1, maps2, add2)


def joint_product(meta, least, index, left, parts, name):
    width = left.shape[1]
    low, high = cuts(width)[index]
    last = high == width
    size = left.shape[0]
    block = 256 if not last else size // 4

    def kernel(meta_ref, left_ref, *refs):
        out_ref = refs[-1]
        part_refs = refs[:-1]

        def times(x):
            total = None
            for (a, b), part in zip(cuts(width), part_refs):
                piece = dot(x[:, a:b], part[0 : b - a, :])
                total = piece if total is None else total + piece
            return total

        @pl.when(meta_ref[0] >= least)
        def _():
            def body(start, count):
                out_ref[pl.ds(start, count), :] = times(left_ref[pl.ds(start, count), :]).astype(BF)

            by_block(size, block, body)
            if last:
                own = part_refs[-1][high - low :, :].astype(F32)
                out_ref[high - low :, :] = (out_ref[high - low :, :].astype(F32) + own).astype(BF)

    return pl.pallas_call(
        kernel,
        out_shape=jax.ShapeDtypeStruct(left.shape, BF),
        in_specs=[SMEM] + [VMEM] * (1 + len(parts)),
        out_specs=VMEM,
        compiler_params=limit(12),
        name=name,
    )(meta, left, *parts)


def begin(meta, maps2, add1, add2):
    def kernel(meta_ref, maps2_ref, add1_ref, add2_ref, out_ref):
        @pl.when(meta_ref[0] == 0)
        def _():
            value = add1_ref[...]

            def body(start, count):
                cols = pl.ds(start, count)
                out_ref[:, cols] = (dot(value, maps2_ref[:, cols]) + add2_ref[:, cols].astype(F32)).astype(BF)

            by_block(maps2_ref.shape[1], 512, body)

        @pl.when(meta_ref[0] != 0)
        def _():
            out_ref[...] = jnp.zeros(out_ref.shape, BF)

    return pl.pallas_call(
        kernel,
        out_shape=jax.ShapeDtypeStruct(add1.shape, BF),
        in_specs=[SMEM] + [VMEM] * 3,
        out_specs=VMEM,
        compiler_params=limit(8),
        name="begin",
    )(meta, maps2, add1, add2)


def advance(meta, position, arrived, maps, kept, out, block):
    def kernel(meta_ref, x_ref, kept_in, out_in, *refs):
        map_refs, (kept_ref, out_ref) = refs[:-2], refs[-2:]

        @pl.when(meta_ref[0] == position)
        def _():
            x = x_ref[...]
            kept_ref[...] = x
            width = x.shape[1]

            def body(start, count):
                cols = pl.ds(start, count)
                out_ref[:, cols] = through(x, [ref.at[:, cols] for ref in map_refs]).astype(BF)

            by_block(width, block, body)

        @pl.when(meta_ref[0] != position)
        def _():
            kept_ref[...] = kept_in[...]
            out_ref[...] = out_in[...]

    operands = list(maps)
    shape = jax.ShapeDtypeStruct(out.shape, BF)
    return pl.pallas_call(
        kernel,
        out_shape=(shape, shape),
        in_specs=[SMEM] + [VMEM] * (3 + len(operands)),
        out_specs=(VMEM, VMEM),
        compiler_params=limit(12),
        name="advance",
    )(meta, arrived, kept, out, *operands)


def late(maps, after, name):
    def kernel(maps_ref, after_ref, out_ref):
        pltpu.sync_copy(maps_ref, out_ref)

    return pl.pallas_call(
        kernel,
        out_shape=jax.ShapeDtypeStruct(maps.shape, BF),
        in_specs=[pl.BlockSpec(memory_space=pl.ANY)] * 2,
        out_specs=pl.BlockSpec(memory_space=pl.ANY),
        compiler_params=limit(8),
        name=name,
    )(maps, after)


def relay(meta, entering, parts):
    def kernel(meta_ref, x_ref, *refs):
        @pl.when((meta_ref[1] == 2) & (meta_ref[0] >= PAIRS))
        def _():
            refs[-1][...] = through(x_ref[...], refs[:-1]).astype(BF)

    return pl.pallas_call(
        kernel,
        out_shape=jax.ShapeDtypeStruct(entering.shape, BF),
        in_specs=[SMEM] + [VMEM] * (1 + len(parts)),
        out_specs=VMEM,
        compiler_params=limit(8),
        name="relay",
    )(meta, entering, *parts)


def two_layers(x, maps1_ref, maps2_ref, add1_ref, add2_ref, first_ref, second_ref):
    def layer(value, maps_ref, add_ref, out_ref):
        def body(start, count):
            cols = pl.ds(start, count)
            out_ref[:, cols] = dot(value, maps_ref[:, cols]) + add_ref[:, cols].astype(F32)

        by_block(maps_ref.shape[1], 512, body)

    layer(x, maps1_ref, add1_ref, first_ref)
    layer(first_ref[...].astype(BF), maps2_ref, add2_ref, second_ref)


def settle_most(meta, chips, kept, near, far, final, maps1, maps2, add1, add2, before1, before2):
    rows, width = kept.shape
    count = len(before1)

    def kernel(meta_ref, kept_ref, near_ref, far_ref, final_ref, m1, m2, a1, a2, *refs):
        part1, part2 = refs[:count], refs[count : 2 * count]
        first_ref, second_ref, x_ref = refs[2 * count :]
        position = meta_ref[0]
        role = meta_ref[1]
        from_near = role == 1

        def enter(parts):
            x = x_ref[...]

            def body(start, count):
                cols = pl.ds(start, count)
                x_ref[:, cols] = through(x, [ref.at[:, cols] for ref in parts]).astype(BF)

            by_block(width, 512, body)

        from_far = (role == 2) & (position >= PAIRS)
        from_final = position == chips - 1

        @pl.when(from_near)
        def _():
            x_ref[...] = near_ref[...]

        @pl.when(from_far)
        def _():
            x_ref[...] = far_ref[...]

        @pl.when(from_final)
        def _():
            x_ref[...] = final_ref[...]

        @pl.when(jnp.logical_not(from_near | from_far | from_final))
        def _():
            x_ref[...] = kept_ref[...]

        @pl.when(role == 4)
        def _():
            enter(part2)

        @pl.when((role == 2) | (role == 4))
        def _():
            enter(part1)

        @pl.when(role != 3)
        def _():
            two_layers(x_ref[...], m1, m2, a1, a2, first_ref, second_ref)

    shape = jax.ShapeDtypeStruct((rows, width), F32)
    return pl.pallas_call(
        kernel,
        out_shape=(shape, shape),
        in_specs=[SMEM] + [VMEM] * (8 + 2 * count),
        out_specs=(VMEM, VMEM),
        scratch_shapes=[pltpu.VMEM((rows, width), BF)],
        compiler_params=limit(16),
        name="settle_most",
    )(meta, kept, near, far, final, maps1, maps2, add1, add2, *before1, *before2)


def settle_third(meta, entering, maps1, maps2, add1, add2, first, second):
    rows, width = entering.shape

    def kernel(meta_ref, x_ref, m1, m2, a1, a2, first_in, second_in, first_ref, second_ref):
        @pl.when(meta_ref[1] == 3)
        def _():
            two_layers(x_ref[...], m1, m2, a1, a2, first_ref, second_ref)

        @pl.when(meta_ref[1] != 3)
        def _():
            first_ref[...] = first_in[...]
            second_ref[...] = second_in[...]

    shape = jax.ShapeDtypeStruct((rows, width), F32)
    return pl.pallas_call(
        kernel,
        out_shape=(shape, shape),
        in_specs=[SMEM] + [VMEM] * 7,
        out_specs=(VMEM, VMEM),
        compiler_params=limit(16),
        name="settle_third",
    )(meta, entering, maps1, maps2, add1, add2, first, second)


def finish(combined, own_add, partner, outer, maps_partner, maps_outer):
    def kernel(c_ref, a_ref, x_ref, o_ref, m1, m2, out_ref):
        part = dot(x_ref[...], m1[...]) + dot(o_ref[...], m2[...])
        out_ref[...] = (a_ref[...].astype(F32) - c_ref[...] + part).astype(BF)

    return pl.pallas_call(
        kernel,
        out_shape=jax.ShapeDtypeStruct(combined.shape, BF),
        in_specs=[VMEM] * 6,
        out_specs=VMEM,
        compiler_params=limit(16),
        name="finish",
    )(combined, own_add, partner, outer, maps_partner, maps_outer)


def shards(down_maps, up_maps, local_traces, src_depth):
    down, up = down_maps[0], up_maps[0]
    rows, width = local_traces.shape
    count = lax.axis_size("layer")
    chips = count // 2
    layer = lax.axis_index("layer")
    core = layer % 2
    chip = layer // 2
    position = jnp.where(core == 1, chip, chips - 1 - chip)
    role = jnp.where(
        position < SINGLES,
        0,
        jnp.where(position < PAIRS, 1 + (position - SINGLES) % 2, 1 + (position - PAIRS) % 4),
    )
    meta = jnp.stack([position, role, core]).astype(jnp.int32)

    def device(at):
        return (2 * at + 1, 2 * (chips - 1 - at))

    def links(steps):
        return [pair for a, b in steps for pair in zip(device(a), device(b))]

    def move(value, steps):
        return lax.ppermute(value, "layer", links(steps))

    partners = [(i, i ^ 1) for i in range(count)]
    zero = jnp.zeros((), BF)
    add2 = jnp.where((src_depth == layer)[:, None], local_traces, zero)
    add1 = jnp.where((src_depth == layer + 1 - 2 * core)[:, None], local_traces, zero)

    down = pltpu.with_memory_space_constraint(down, pltpu.HBM)
    up = pltpu.with_memory_space_constraint(up, pltpu.HBM)
    given = pick(meta, down, up, "pick_given")
    maps2 = pick(meta, up, down, "pick_own")
    maps1 = lax.ppermute(given, "layer", partners)
    thirds = range(len(cuts(width)))
    one = [chip_product(meta, EARLY, i, maps1, add1, maps2, add2) for i in thirds]
    pairs = [(e, e + 1) for e in range(SINGLES, chips, 2)]
    before1 = [move(part, pairs) for part in one]
    two = [joint_product(meta, SINGLES, i, before1[i], one, "pair_product") for i in thirds]
    quads = range(PAIRS, chips, 4)
    before2 = [move(part, [(e + 1, e + 3) for e in quads]) for part in two]
    four = [joint_product(meta, PAIRS, i, before2[i], two, "quad_product") for i in thirds]

    stops = [(at, one) for at in range(EARLY, SINGLES)]
    stops += [(e + 1, two) for e in range(SINGLES, PAIRS, 2)]
    stops += [(e + 3, four) for e in range(PAIRS, chips - 4, 4)]
    kept = jnp.zeros((rows, width), BF)
    out = begin(meta, maps2, add1, add2)
    last = 0
    for at, maps in stops:
        arrived = move(out, [(last, at)])
        if at == stops[-2][0]:
            ahead = out
        kept, out = advance(meta, at, arrived, maps, kept, out, width if maps is four else 512)
        last = at

    far = move(out, [(e - 1, e + 1) for e in quads])
    final = move(out, [(last, chips - 1)])
    near = move(out, [(e - 1, e) for e in list(range(SINGLES, PAIRS, 2)) + list(quads)])
    maps1 = late(maps1, ahead, "late_first")
    given = pick(meta, down, up, "late_given", ahead)
    passed = move(relay(meta, far, two), [(e + 1, e + 2) for e in quads])
    first, second = settle_most(
        meta, chips, kept, near, far, final, maps1, maps2, add1, add2, before1, before2
    )
    first, second = settle_third(meta, passed, maps1, maps2, add1, add2, first, second)

    combined = second + lax.ppermute(first, "layer", partners) - add2.astype(F32)
    rounded = combined.astype(BF)
    partner = lax.ppermute(rounded, "layer", partners)
    outward = [(i, i + 1) for i in range(1, count - 1, 2)]
    outer = lax.ppermute(rounded, "layer", outward + [(b, a) for a, b in outward])
    residual = finish(combined, add2, partner, outer, maps2, given)
    return (rounded[None], residual[None])


def solution(mesh):
    placed = (P("layer", None, None), P("layer", None, None), P("src", None), P("src"))
    return jax.shard_map(
        shards,
        mesh=mesh,
        in_specs=placed,
        out_specs=(P("layer", "src", None), P("layer", "src", None)),
        check_vma=False,
    )
```
